32 devices in a mesh: curve: 8 (over z, x), head: 4 (over y, core).
Axes of the slice: x: 2, y: 2, z: 4, core: 2. Of those that a mesh axis runs over, the one named last changes fastest.
Arguments:
- points: bfloat16 [16384, 1024], P(('curve', 'head')), may hold values from -6 to 6
- order: int32 [32, 512], P(('curve', 'head')), may hold values from 0 to 511, each once within a row
- scan_ids: int32 [16384], P(('curve', 'head')), may hold values from 0 to 3
- ln_gain: float32 [2, 1024], replicated, may hold values from 0.25 to 1.75
- w_qkv: bfloat16 [2, 1024, 3072], P(None, None, 'head'), may hold values from -7 to 7, as said below
- w_out: bfloat16 [2, 1024, 1024], P(None, 'head'), may hold values from -0.1875 to 0.1875
Outputs:
- refined: bfloat16 [16384, 1024], P(('curve', 'head'))
The draws below stay inside these ranges and needn't reach their ends.
Inputs may be any that keep to these rules, and one draw needn't show every extreme that they name: `order`: row b is a permutation of the 512 rows of block b. `w_qkv`: columns ordered by head, then query, key, value, then entry.
All inputs are finite; a program needn't handle non-finite values.
Results may differ from the reference program's by a relative error of at most 0.01.
Values may be sent and summed in bfloat16 or wider, within the bound.
A program may use at most 64 MiB of HBM per device.

```python
import jax
import jax.numpy as jnp
from jax import lax

D = 1024
HEADS = 16
HEAD_DIM = 64
PATCH = 1024
SCANS = 4
TOK_DEV = 512
TOKENS = 16384
DEVICES = 32


def draw_w_qkv(key, part):
    base = jnp.clip(jax.random.normal(key, (2, D, HEADS, 3, HEAD_DIM), jnp.float32), -5.0, 5.0) * D ** (-0.5)
    return base.reshape(2, D, HEADS * 3 * HEAD_DIM).astype(jnp.bfloat16)


def touch_ends(values, own_key, smallest, largest):
    longest = values.shape.index(max(values.shape))
    spots = []
    for shift in (0, 1):
        where = [jax.random.randint(jax.random.fold_in(own_key, axis), (), 0, length) for axis, length in enumerate(values.shape)]
        where[longest] = (where[longest] + shift) % values.shape[longest]
        spots.append(tuple(where))
    return values.at[spots[0]].set(smallest).at[spots[1]].set(largest)


def level_of(own_key, extent, pieces, smallest, largest):
    def one(axis_at, blocks):
        heights = jax.random.uniform(jax.random.fold_in(jax.random.fold_in(own_key, 6), axis_at), (blocks,), jnp.float32, smallest / len(pieces), largest / len(pieces))
        return jnp.repeat(jnp.exp(heights), extent[axis_at] // blocks).reshape((-1,) + (1,) * (len(extent) - axis_at - 1))

    factor_of = one(*pieces[0])
    for cut in pieces[1:]:
        factor_of = factor_of * one(*cut)
    return factor_of


def normal_values(rng, extent, scale, most, split=(), held_as=jnp.bfloat16):
    level = level_of(rng, extent, split, -0.22, 0.18) if split else 1.0
    result = jax.random.normal(rng, extent, jnp.float32) * scale * level
    return jnp.minimum(jnp.maximum(result, -most), most).astype(held_as)


def setup_inputs(seed: int = 0) -> dict:
    splits = jax.random.split(jax.random.key(seed), 7)
    return {
        "points": normal_values(splits[0], (TOKENS, D), 1.0, 6.0, ((0, 32),)),
        "order": jax.vmap(lambda own: jax.random.permutation(own, TOK_DEV))(jax.random.split(splits[1], DEVICES)).reshape((DEVICES, TOK_DEV)).astype(jnp.int32),
        "scan_ids": touch_ends(jax.random.randint(splits[2], (TOKENS,), 0, SCANS), jax.random.fold_in(splits[2], 1), 0, SCANS - 1).astype(jnp.int32),
        "ln_gain": jnp.clip(1.0 + 0.15 * jax.random.normal(splits[3], (2, D), jnp.float32), 0.25, 1.75),
        "w_qkv": draw_w_qkv(jax.random.fold_in(splits[6], 71), 0),
        "w_out": normal_values(splits[5], (2, D, D), D ** -0.5, 0.1875, ((1, 4),)),
    }


EPSILON = 1e-05

def layer_norm(rows, gain):
    values = rows.astype(jnp.float32)
    center = values - lax.optimization_barrier(jnp.mean(values, axis=-1, keepdims=True))
    spread = lax.optimization_barrier(jnp.mean(center * center, axis=-1, keepdims=True))
    return (center * lax.rsqrt(spread + EPSILON) * gain.astype(jnp.float32)).astype(jnp.bfloat16)

def window_attention(qkv_all, tags, offset):
    length = qkv_all.shape[0]
    rolled = jnp.roll(qkv_all, -offset, axis=0)
    rolled_tags = jnp.roll(tags, -offset, axis=0)
    windows = length // PATCH
    parts = rolled.reshape(windows, PATCH, HEADS, 3, HEAD_DIM)
    part_tags = rolled_tags.reshape(windows, PATCH)

    def one_window(inputs):
        piece, piece_tags = inputs
        queries = piece[:, :, 0].astype(jnp.float32)
        keys = piece[:, :, 1].astype(jnp.float32)
        values = piece[:, :, 2].astype(jnp.float32)
        scores = jnp.einsum('qhd,khd->hqk', queries, keys) * HEAD_DIM ** (-0.5)
        allowed = piece_tags[:, None] == piece_tags[None, :]
        scores = jnp.where(allowed[None], scores, -jnp.inf)
        row_max = lax.optimization_barrier(jnp.max(scores, axis=-1, keepdims=True))
        expo = jnp.exp(scores - row_max)
        probs = (expo / lax.optimization_barrier(jnp.sum(expo, axis=-1, keepdims=True))).astype(jnp.bfloat16)
        heads = jnp.einsum('hqk,khd->qhd', probs.astype(jnp.float32), values)
        return heads.astype(jnp.bfloat16)
    outputs = lax.map(one_window, (parts, part_tags))
    return jnp.roll(outputs.reshape(length, HEADS * HEAD_DIM), offset, axis=0)

def reference(points, order, scan_ids, ln_gain, w_qkv, w_out):
    blocks = points.reshape(-1, TOK_DEV, D)
    stream = jax.vmap(lambda block, picks: block[picks])(blocks, order.astype(jnp.int32)).reshape(-1, D)
    for layer_index in range(2):
        normed = layer_norm(stream, ln_gain[layer_index])
        qkv_all = jnp.dot(normed, w_qkv[layer_index], preferred_element_type=jnp.float32).astype(jnp.bfloat16)
        heads = window_attention(qkv_all, scan_ids, layer_index * (PATCH // 2))
        update = jnp.dot(heads, w_out[layer_index], preferred_element_type=jnp.float32)
        stream = (stream.astype(jnp.float32) + update).astype(jnp.bfloat16)
    return stream
```

```python
import functools

import jax
import jax.numpy as jnp
from jax import lax
from jax.experimental import pallas as pl
from jax.experimental.pallas import tpu as pltpu
from jax.sharding import PartitionSpec as P

HEAD_DIM = 64
PATCH = 1024


EPSILON = 1e-05


def extended(array, sides, width):
    for axis, dim in sides:
        peers, length = (lax.axis_size(axis), array.shape[dim])
        up = [(i, (i + 1) % peers) for i in range(peers)]
        down = [(j, i) for i, j in up]
        last = lax.slice_in_dim(array, length - width, length, axis=dim)
        first = lax.slice_in_dim(array, 0, width, axis=dim)
        before = lax.ppermute(last, axis, up)
        after = lax.ppermute(first, axis, down)
        array = jnp.concatenate([before, array, after], axis=dim)
    return array


def layer_norm(rows, gain):
    values = rows.astype(jnp.float32)
    center = values - jnp.mean(values, axis=-1, keepdims=True)
    spread = jnp.mean(center * center, axis=-1, keepdims=True)
    return (center * lax.rsqrt(spread + EPSILON) * gain).astype(jnp.bfloat16)


def attend_block(heads_local, kv_stride, k_at, q_ref, kv_ref, qt_ref, kt_ref, out_ref):
    rows = q_ref.shape[0]
    keys = kv_ref.shape[0]
    bias = jnp.where(qt_ref[...] == kt_ref[...], 0.0, -jnp.inf)
    ones = jnp.ones((keys, HEAD_DIM), jnp.bfloat16)
    for head in range(heads_local):
        q_at = head * 3 * HEAD_DIM
        key_at = head * kv_stride + k_at
        query = q_ref[:, q_at : q_at + HEAD_DIM] * jnp.bfloat16(HEAD_DIM ** (-0.5))
        key = kv_ref[:, key_at : key_at + HEAD_DIM]
        value = kv_ref[:, key_at + HEAD_DIM : key_at + 2 * HEAD_DIM]
        scores = lax.dot_general(
            query, key, (((1,), (1,)), ((), ())), preferred_element_type=jnp.float32
        ) + bias
        row_max = jnp.max(scores, axis=-1, keepdims=True)
        expo = jnp.exp(scores - row_max).astype(jnp.bfloat16)
        result = jnp.dot(
            expo, jnp.concatenate([value, ones], axis=1), preferred_element_type=jnp.float32
        )
        normal = result[:, :HEAD_DIM] / result[:, HEAD_DIM : HEAD_DIM + 1]
        out_ref[:, head * HEAD_DIM : (head + 1) * HEAD_DIM] = normal.astype(jnp.bfloat16)


def attend(queries, kv, query_tags, key_tags, kv_stride, k_at, centred):
    block_rows = PATCH // 2
    span, width = queries.shape
    heads_local = width // (3 * HEAD_DIM)
    shift = 1 if centred else 0
    return pl.pallas_call(
        functools.partial(attend_block, heads_local, kv_stride, k_at),
        grid=(span // block_rows,),
        out_shape=jax.ShapeDtypeStruct((span, heads_local * HEAD_DIM), jnp.bfloat16),
        in_specs=[
            pl.BlockSpec((block_rows, width), lambda i: (i, 0)),
            pl.BlockSpec((PATCH, kv.shape[1]), lambda i: ((i + shift) // 2, 0)),
            pl.BlockSpec((block_rows, 1), lambda i: (i, 0)),
            pl.BlockSpec((1, PATCH), lambda i: (0, (i + shift) // 2)),
        ],
        out_specs=pl.BlockSpec((block_rows, heads_local * HEAD_DIM), lambda i: (i, 0)),
        cost_estimate=pl.CostEstimate(
            flops=4 * span * PATCH * heads_local * HEAD_DIM,
            bytes_accessed=span * width * 8,
            transcendentals=span * PATCH * heads_local,
        ),
    )(queries, kv, query_tags.reshape(-1, 1), key_tags.reshape(1, -1))


def on_device(points, order, scan_ids, ln_gain, w_qkv, w_out):
    stream = points[order[0]]
    range_ids = lax.all_gather(scan_ids, "head", axis=0, tiled=True)
    span_rows = range_ids.shape[0]
    heads_local = w_qkv.shape[2] // (3 * HEAD_DIM)
    half_patch = PATCH // 2
    for layer_index in range(2):
        normed = layer_norm(stream, ln_gain[layer_index])
        weights_here = w_qkv[layer_index]
        qkv_span = jnp.dot(
            lax.all_gather(normed, "head", axis=0, tiled=True),
            weights_here,
            preferred_element_type=jnp.float32,
        ).astype(jnp.bfloat16)
        if layer_index == 0:
            attended = attend(
                qkv_span, qkv_span, range_ids, range_ids, 3 * HEAD_DIM, HEAD_DIM, False
            )
        else:
            tags_float = range_ids.astype(jnp.bfloat16)
            kv_flat = qkv_span.reshape(span_rows, heads_local, 3, HEAD_DIM)[:, :, 1:].reshape(
                span_rows, heads_local * 2 * HEAD_DIM
            )
            wide_kv, wide_tags = (
                extended(kv_flat, (("curve", 0),), half_patch),
                extended(tags_float, (("curve", 0),), half_patch),
            )
            attended = attend(
                qkv_span,
                wide_kv,
                range_ids,
                wide_tags.astype(jnp.int32),
                2 * HEAD_DIM,
                0,
                True,
            )
        heads_rows = lax.all_to_all(attended, "head", split_axis=0, concat_axis=1, tiled=True)
        update = jnp.dot(
            heads_rows,
            lax.all_gather(w_out[layer_index], "head", axis=0, tiled=True),
            preferred_element_type=jnp.float32,
        )
        stream = (stream.astype(jnp.float32) + update).astype(jnp.bfloat16)
    return stream


def solution(mesh):
    in_specs = (
        P(("curve", "head"), None),
        P(("curve", "head"), None),
        P(("curve", "head")),
        P(),
        P(None, None, "head"),
        P(None, "head", None),
    )
    out_specs = P(("curve", "head"), None)
    return jax.shard_map(
        on_device, mesh=mesh, in_specs=in_specs, out_specs=out_specs, check_vma=False
    )
```

```python
import functools

import jax
import jax.numpy as jnp
from jax import lax
from jax.experimental import pallas as pl
from jax.experimental.pallas import tpu as pltpu
from jax.sharding import PartitionSpec as P

HEAD_DIM = 64
PATCH = 1024


EPSILON = 1e-05


def layer_norm(rows, gain):
    values = rows.astype(jnp.float32)
    center = values - jnp.mean(values, axis=-1, keepdims=True)
    spread = jnp.mean(center * center, axis=-1, keepdims=True)
    return (center * lax.rsqrt(spread + EPSILON) * gain).astype(jnp.bfloat16)


def remote(src, dst, send_sem, recv_sem, device):
    return pltpu.make_async_remote_copy(
        src_ref=src,
        dst_ref=dst,
        send_sem=send_sem,
        recv_sem=recv_sem,
        device_id=device,
        device_id_type=pl.DeviceIdType.MESH,
    )


def layer_kernel(
    peers, ranges, halo, x_ref, tag_ref, w_ref, wo_ref, stream_ref, out_ref,
    all_x, q_buf, kv_buf, tags, att, heads, all_wo,
    x_recv, x_send, w_recv, w_send, t_recv, t_send, h_recv, h_send, kv_recv, kv_send,
):
    chunks, chunk_rows, _ = x_ref.shape
    rows = chunks * chunk_rows
    heads_local = w_ref.shape[1] // (3 * HEAD_DIM)
    chips = peers // 2
    window_blocks = PATCH // rows
    curve = lax.axis_index("curve")
    me = lax.axis_index("head")
    chip, core = me // 2, me % 2
    partner = chip * 2 + 1 - core
    up, down = {"curve": (curve + 1) % ranges}, {"curve": (curve + ranges - 1) % ranges}
    same = [((chip + s) % chips) * 2 + core for s in range(chips)]
    other = [((chip + s) % chips) * 2 + 1 - core for s in range(chips)]
    others = [(me + t) % peers for t in range(1, peers)]

    barrier = pltpu.get_barrier_semaphore()
    for blk in others:
        pl.semaphore_signal(
            barrier, inc=1, device_id={"head": blk}, device_id_type=pl.DeviceIdType.MESH
        )
    if halo:
        for neighbour in (up, down):
            pl.semaphore_signal(
                barrier, inc=1, device_id=neighbour, device_id_type=pl.DeviceIdType.MESH
            )
    pl.semaphore_wait(barrier, peers - 1 + (2 if halo else 0))

    def direct_x(s, c):
        dest = partner if s == 0 else same[s]
        return remote(
            x_ref.at[c], all_x.at[me, c], x_send.at[s, c], x_recv.at[me, c], {"head": dest}
        )

    def passed_x(s, c):
        part = all_x.at[same[s], c]
        return remote(
            part, part, x_send.at[chips + s, c], x_recv.at[same[s], c], {"head": partner}
        )

    def wait_x(blk, c):
        part = all_x.at[blk, c]
        remote(part, part, x_send.at[0, c], x_recv.at[blk, c], {"head": partner}).wait_recv()

    def tag_copy(t):
        return remote(
            tag_ref.at[0], tags.at[halo + me], t_send.at[t], t_recv.at[halo + me],
            {"head": others[t]},
        )

    def direct_w(s):
        dest = partner if s == 0 else same[s]
        return remote(wo_ref, all_wo.at[me], w_send.at[s], w_recv.at[me], {"head": dest})

    def passed_w(s):
        part = all_wo.at[same[s]]
        return remote(
            part, part, w_send.at[chips + s], w_recv.at[same[s]], {"head": partner}
        )

    def wait_w(blk):
        part = all_wo.at[blk]
        remote(part, part, w_send.at[0], w_recv.at[blk], {"head": partner}).wait_recv()

    def edge(buffer, send, recv, j):
        if j < halo:
            src, dst, device = buffer.at[peers + j], buffer.at[j], up
        else:
            src, dst, device = buffer.at[j], buffer.at[peers + j], down
        return remote(src, dst, send.at[j], recv.at[j], device)

    tag_send_edge = peers - 1

    for s in range(chips):
        for c in range(chunks):
            direct_x(s, c).start()
    for t in range(peers - 1):
        tag_copy(t).start()
    direct_w(0).start()
    tags[halo + me] = tag_ref[0]

    def project(values, blk, first_row):
        result = jnp.dot(values, w_ref[...], preferred_element_type=jnp.float32)
        result = result.astype(jnp.bfloat16)
        at = pl.ds(first_row, chunk_rows)
        for head in range(heads_local):
            base = head * 3 * HEAD_DIM
            q_buf[blk, at, head * HEAD_DIM : (head + 1) * HEAD_DIM] = result[
                :, base : base + HEAD_DIM
            ] * jnp.bfloat16(HEAD_DIM ** (-0.5))
            kv_buf[halo + blk, at, head * 2 * HEAD_DIM : (head + 1) * 2 * HEAD_DIM] = result[
                :, base + HEAD_DIM : base + 3 * HEAD_DIM
            ]

    def project_block(blk):
        for c in range(chunks):
            project(all_x[blk, c], blk, c * chunk_rows)

    def attend(blk):
        first = (blk + halo) // window_blocks * window_blocks
        column = jnp.transpose(
            jnp.broadcast_to(tags[halo + blk].astype(jnp.float32), (128, rows))
        )[:, :1]
        line = jnp.concatenate(
            [tags[first + j].astype(jnp.float32) for j in range(window_blocks)], axis=1
        )
        bias = jnp.where(column == line, 0.0, -jnp.inf)
        ones = jnp.ones((PATCH, HEAD_DIM), jnp.bfloat16)
        for head in range(heads_local):
            at = head * 2 * HEAD_DIM
            wide = kv_buf[pl.ds(first, window_blocks), :, at : at + 2 * HEAD_DIM].reshape(
                PATCH, 2 * HEAD_DIM
            )
            query = q_buf[blk, :, head * HEAD_DIM : (head + 1) * HEAD_DIM]
            scores = lax.dot_general(
                query, wide[:, :HEAD_DIM], (((1,), (1,)), ((), ())),
                preferred_element_type=jnp.float32,
            ) + bias
            row_max = jnp.max(scores, axis=-1, keepdims=True)
            expo = jnp.exp(scores - row_max).astype(jnp.bfloat16)
            result = jnp.dot(
                expo,
                jnp.concatenate([wide[:, HEAD_DIM:], ones], axis=1),
                preferred_element_type=jnp.float32,
            )
            normal = result[:, :HEAD_DIM] / result[:, HEAD_DIM : HEAD_DIM + 1]
            att[blk, :, head * HEAD_DIM : (head + 1) * HEAD_DIM] = normal.astype(jnp.bfloat16)

    def head_copy(t):
        blk = others[t]
        return remote(
            att.at[blk], heads.at[me], h_send.at[t], h_recv.at[me], {"head": blk}
        )

    def head_copy_to(blk):
        t = (blk - me + peers - 1) % peers
        return remote(
            att.at[blk], heads.at[me], h_send.at[t], h_recv.at[me], {"head": blk}
        )

    for c in range(chunks):
        project(x_ref[c], me, c * chunk_rows)
    for c in range(chunks):
        wait_x(partner, c)
    project_block(partner)
    for blk in others:
        part = tags.at[halo + blk]
        remote(part, part, t_send.at[0], t_recv.at[halo + blk], {"head": partner}).wait_recv()
    if halo:
        for j in range(2 * halo):
            edge(tags, t_send.at[pl.ds(peers, 2 * halo)], t_recv.at[pl.ds(peers + 2 * halo, 2 * halo)], j).start()

    early = not halo and window_blocks == 2
    if early:
        attend(me)
        attend(partner)
        head_copy_to(partner).start()
    for s in range(1, chips):
        for c in range(chunks):
            wait_x(same[s], c)
            passed_x(s, c).start()
            project(all_x[same[s], c], same[s], c * chunk_rows)
    for s in range(1, chips):
        direct_w(s).start()
        for c in range(chunks):
            wait_x(other[s], c)
            project(all_x[other[s], c], other[s], c * chunk_rows)
    if halo:
        for j in range(2 * halo):
            edge(kv_buf, kv_send, kv_recv, j).start()
        middle = chips // 2 if window_blocks == 2 else 0
        for j in range(2 * halo):
            edge(tags, t_send.at[pl.ds(peers, 2 * halo)], t_recv.at[pl.ds(peers + 2 * halo, 2 * halo)], j).wait_recv()

    def finish(blk):
        attend(blk)

        @pl.when(blk != me)
        def _():
            head_copy_to(blk).start()

    if early:
        for s in range(1, chips):
            finish(other[s])
            finish(same[s])
    else:
        if halo:
            inner = list(range(halo, peers - halo))
            outer = list(range(peers - halo, peers)) + list(range(halo))

            def inner_step(i, carry):
                finish(halo + (me + 1 + i) % (peers - 2 * halo))
                return carry

            lax.fori_loop(0, len(inner), inner_step, 0)
            for j in range(2 * halo):
                edge(kv_buf, kv_send, kv_recv, j).wait_recv()

            def outer_step(i, carry):
                finish((peers - halo + (me + i) % (2 * halo)) % peers)
                return carry

            lax.fori_loop(0, len(outer), outer_step, 0)
        else:

            def step(i, carry):
                finish((me + 1 + i) % peers)
                return carry

            lax.fori_loop(0, peers, step, 0)

    wait_w(partner)
    for s in range(1, chips):
        wait_w(same[s])
        passed_w(s).start()
    heads[me] = att[me]
    all_wo[me] = wo_ref[...]
    for s in range(1, chips):
        wait_w(other[s])
    for blk in others:
        part = heads.at[blk]
        remote(part, part, h_send.at[0], h_recv.at[blk], {"head": partner}).wait_recv()

    for c in range(chunks):
        at = pl.ds(c * chunk_rows, chunk_rows)
        total = stream_ref[at, :].astype(jnp.float32)
        for blk in range(peers):
            total += jnp.dot(
                heads[blk, at, :], all_wo[blk], preferred_element_type=jnp.float32
            )
        out_ref[at, :] = total.astype(jnp.bfloat16)

    for s in range(chips):
        for c in range(chunks):
            direct_x(s, c).wait_send()
            if s:
                passed_x(s, c).wait_send()
        direct_w(s).wait_send()
        if s:
            passed_w(s).wait_send()
    for t in range(peers - 1):
        tag_copy(t).wait_send()
        head_copy(t).wait_send()
    for j in range(2 * halo):
        edge(tags, t_send.at[pl.ds(peers, 2 * halo)], t_recv.at[pl.ds(peers + 2 * halo, 2 * halo)], j).wait_send()
        edge(kv_buf, kv_send, kv_recv, j).wait_send()


def layer(index, stream, normed, tag_row, weights, out_weights):
    rows, width = stream.shape
    peers, ranges = lax.axis_size("head"), lax.axis_size("curve")
    halo = PATCH // 2 // rows if index else 0
    chips = peers // 2
    chunks = max(1, rows // 256)
    columns = out_weights.shape[0]
    vmem = pl.BlockSpec(memory_space=pltpu.VMEM)
    dma = pltpu.SemaphoreType.DMA
    bf16 = jnp.bfloat16
    return pl.pallas_call(
        functools.partial(layer_kernel, peers, ranges, halo),
        out_shape=jax.ShapeDtypeStruct((rows, width), bf16),
        in_specs=[vmem] * 5,
        out_specs=vmem,
        scratch_shapes=[
            pltpu.VMEM((peers, chunks, rows // chunks, width), bf16),
            pltpu.VMEM((peers, rows, columns), bf16),
            pltpu.VMEM((peers + 2 * halo, rows, 2 * columns), bf16),
            pltpu.VMEM((peers + 2 * halo, 1, rows), jnp.int32),
            pltpu.VMEM((peers, rows, columns), bf16),
            pltpu.VMEM((peers, rows, columns), bf16),
            pltpu.VMEM((peers, columns, width), bf16),
            dma((peers, chunks)),
            dma((peers, chunks)),
            dma((peers,)),
            dma((peers,)),
            dma((peers + 4 * halo,)),
            dma((peers + 2 * halo,)),
            dma((peers,)),
            dma((peers,)),
            dma((max(1, 2 * halo),)),
            dma((max(1, 2 * halo),)),
        ],
        compiler_params=pltpu.CompilerParams(collective_id=index, has_side_effects=True),
        cost_estimate=pl.CostEstimate(
            flops=20 * rows * width * width, bytes_accessed=20 * rows * width, transcendentals=0
        ),
    )(
        normed.reshape(chunks, rows // chunks, width),
        tag_row,
        weights,
        out_weights,
        stream,
    )


def on_device(points, order, scan_ids, ln_gain, w_qkv, w_out):
    stream = points[order[0]]
    tag_row = scan_ids.reshape(1, 1, -1)
    for index in range(2):
        normed = layer_norm(stream, ln_gain[index])
        stream = layer(index, stream, normed, tag_row, w_qkv[index], w_out[index])
    return stream


def solution(mesh):
    in_specs = (
        P(("curve", "head"), None),
        P(("curve", "head"), None),
        P(("curve", "head")),
        P(),
        P(None, None, "head"),
        P(None, "head", None),
    )
    out_specs = P(("curve", "head"), None)
    return jax.shard_map(
        on_device, mesh=mesh, in_specs=in_specs, out_specs=out_specs, check_vma=False
    )
```
